1024 devices in a mesh: circ: 32 (over x_hi, z), rad: 16 (over y, x_lo), ax: 2 (over core).
Axes of the slice: x: 8 (x_hi: 4, x_lo: 2; x = x_hi * 2 + x_lo), y: 8, z: 8, core: 2. Of those that a mesh axis runs over, the one named last changes fastest.
Arguments:
- state: float32 [5, 16, 128, 4096], P(None, 'ax', 'rad', 'circ'), may hold values from -6 to 6
- eddy: float32 [16, 128, 4096], P('ax', 'rad', 'circ'), may hold values from 0.02 to 0.2
- offsets: int32 [4], replicated, may hold values from 0 to 31, as said below
- stencil_index: int32 [2, 4, 128, 4], replicated, may hold values from 0 to 127
- stencil_weight: float32 [2, 4, 128, 4], replicated, may hold values from 0.1 to 1
Outputs:
- advanced: float32 [5, 16, 128, 4096], P(None, 'ax', 'rad', 'circ')
The draws below stay inside these ranges and needn't reach their ends.
Inputs may be any that keep to these rules, and one draw needn't show every extreme that they name: Among the sections' offsets are 16, 31 and 0.
All inputs are finite; a program needn't handle non-finite values.
Results may differ from the reference program's by a relative error of at most 0.00005.
Values sent between devices are 32-bit elements; how exact they have to be, the bound alone decides.
No kernel may reach another device: no remote copies, remote signals or barrier semaphores. Data moves between devices by JAX's collectives and lax.ppermute only.
A program may use at most 32 MiB of HBM per device.

```python
import math
import jax
import jax.numpy as jnp
from jax import lax

NV = 5
SECTIONS = 4
TAPS = 4
CC = 128
CA = 8
NC = 4096
NR = 128
NA = 16
N_CIRC = 32


def draw_offsets(key, part):
    values = jax.random.randint(jax.random.fold_in(key, 11), (SECTIONS,), 0, N_CIRC, dtype=jnp.int32)
    chosen = jax.random.randint(jax.random.fold_in(key, 12), (), 0, SECTIONS, dtype=jnp.int32)
    section_ids = jnp.arange(SECTIONS, dtype=jnp.int32)
    after_one = (chosen + 1) % SECTIONS
    after_two = (chosen + 2) % SECTIONS
    values = jnp.where(section_ids == after_two, jnp.int32(0), values)
    values = jnp.where(section_ids == after_one, jnp.int32(N_CIRC - 1), values)
    values = jnp.where(section_ids == chosen, jnp.int32(N_CIRC // 2), values)
    return values.astype(jnp.int32)


def set_ends(values, key, least, largest):
    place = [jax.random.randint(jax.random.fold_in(key, axis), (), 0, length) for axis, length in enumerate(values.shape)]
    widest = values.shape.index(max(values.shape))
    neighbour = place[:widest] + [(place[widest] + 1) % values.shape[widest]] + place[widest + 1:]
    return values.at[tuple(place)].set(least).at[tuple(neighbour)].set(largest)


def shard_levels(key, shape, shards, least, top_value):
    gain, own = 1.0, jax.random.fold_in(key, 6)
    for axis_at, parts in shards:
        steps = jnp.exp(jax.random.uniform(jax.random.fold_in(own, axis_at), (parts,), jnp.float32, least / len(shards), top_value / len(shards)))
        gain = gain * jnp.repeat(steps, shape[axis_at] // parts).reshape([-1 if axis == axis_at else 1 for axis in range(len(shape))])
    return gain


def bell_draw(rng, extent, scale, most, pieces=(), kind=jnp.bfloat16):
    gain = shard_levels(rng, extent, pieces, -0.22, 0.18) if pieces else 1.0
    drawn = jax.random.normal(rng, extent, jnp.float32) * scale * gain
    return jnp.minimum(jnp.maximum(drawn, -most), most).astype(kind)


def setup_inputs(seed: int = 0) -> dict:
    splits = jax.random.split(jax.random.key(seed), 6)
    state = bell_draw(splits[0], (NV, NA, NR, NC), 1.0, 6.0, ((1, 2), (2, 16), (3, 32)), jnp.float32)
    eddy = jnp.clip(jnp.exp(math.log(0.2) - 2.3025851 * jax.random.uniform(splits[1], (NA, NR, NC), jnp.float32) ** shard_levels(splits[1], (NA, NR, NC), ((0, 2), (1, 16), (2, 32)), -0.2, 0.2)), 0.02, 0.2)
    offsets = draw_offsets(jax.random.fold_in(splits[5], 71), 0)
    stencil_index = set_ends(jax.random.randint(splits[3], (2, SECTIONS, CC, TAPS), 0, CC), jax.random.fold_in(splits[3], 1), 0, CC - 1).astype(jnp.int32)
    stencil_weight = jnp.clip(jax.random.uniform(splits[4], (2, SECTIONS, CC, TAPS), jnp.float32, 0.1, 1.0), 0.1, 1.0)
    return dict(state=state, eddy=eddy, offsets=offsets, stencil_index=stencil_index, stencil_weight=stencil_weight)


AXIAL_MACH = 0.4
STEP_SIZE = 0.3


def interp_matrix(index_rows, weight_rows):
    width = index_rows.shape[0]
    onehot = (index_rows[:, :, None] == jnp.arange(width, dtype=jnp.int32)[None, None, :]).astype(jnp.float32)
    normed = weight_rows / jnp.sum(weight_rows, axis=1, keepdims=True)
    return jnp.sum(normed[:, :, None] * onehot, axis=1)


def tendency(center, circ_low, circ_high, radial_low, radial_high, axial_low, axial_high, swirl, eddy):
    diff_circ = 0.5 * (circ_high - circ_low)
    diff_radial = 0.5 * (radial_high - radial_low)
    diff_axial = 0.5 * (axial_high - axial_low)
    laplace = (circ_high + circ_low) + (radial_high + radial_low) + (axial_high + axial_low) - 6.0 * center
    advect = swirl * diff_circ + AXIAL_MACH * diff_axial
    diverge = diff_circ[1] + diff_radial[2] + diff_axial[3]
    flux = jnp.stack([diverge, diff_circ[4], diff_radial[4], diff_axial[4], diverge])
    return -advect - flux + eddy[None] * laplace


def interpolate(plane, matrix):
    width = matrix.shape[0]
    flat_rows = plane.reshape(-1, width)
    out = jnp.dot(flat_rows, matrix.T, precision=lax.Precision.HIGHEST, preferred_element_type=jnp.float32)
    return out.reshape(plane.shape)


def section_tendency(field, eddy, offset_now, index_section, weight_section):
    sectors = N_CIRC
    nvar, naxial, nradial, ncirc = field.shape
    stator_plane = field[:, CA - 1].reshape(nvar, nradial, sectors, CC)
    rotor_plane = field[:, CA].reshape(nvar, nradial, sectors, CC)
    cycle = jnp.arange(sectors, dtype=jnp.int32)
    facing_rotor = stator_plane[:, :, (cycle + offset_now) % sectors]
    facing_stator = rotor_plane[:, :, (cycle + sectors - offset_now) % sectors]
    rotor_ghost = interpolate(facing_rotor, interp_matrix(index_section[1], weight_section[1])).reshape(nvar, nradial, ncirc)
    stator_ghost = interpolate(facing_stator, interp_matrix(index_section[0], weight_section[0])).reshape(nvar, nradial, ncirc)
    circ_low = jnp.roll(field, 1, axis=3)
    circ_high = jnp.roll(field, -1, axis=3)
    zero_row = jnp.zeros((nvar, naxial, 1, ncirc), jnp.float32)
    radial_low = jnp.concatenate([zero_row, field[:, :, :-1]], axis=2)
    radial_high = jnp.concatenate([field[:, :, 1:], zero_row], axis=2)
    zero_plane = jnp.zeros((nvar, 1, nradial, ncirc), jnp.float32)
    results = []
    for half in range(2):
        lower = half * CA
        block = field[:, lower:lower + CA]
        if half == 0:
            below, above, swirl = zero_plane, stator_ghost[:, None], 0.2
        else:
            below, above, swirl = rotor_ghost[:, None], zero_plane, -0.3
        axial_low = jnp.concatenate([below, block[:, :-1]], axis=1)
        axial_high = jnp.concatenate([block[:, 1:], above], axis=1)
        results.append(tendency(block, circ_low[:, lower:lower + CA], circ_high[:, lower:lower + CA],
                                radial_low[:, lower:lower + CA], radial_high[:, lower:lower + CA],
                                axial_low, axial_high, swirl, eddy[lower:lower + CA]))
    return jnp.concatenate(results, axis=1)


def reference(state, eddy, offsets, stencil_index, stencil_weight):
    def slope(field, section):
        return section_tendency(field, eddy, offsets[section], stencil_index[:, section], stencil_weight[:, section])

    slope_one = slope(state, 0)
    slope_two = slope(state + (0.5 * STEP_SIZE) * slope_one, 1)
    slope_three = slope(state + (0.5 * STEP_SIZE) * slope_two, 2)
    slope_four = slope(state + STEP_SIZE * slope_three, 3)
    return state + (STEP_SIZE / 6.0) * (slope_one + 2.0 * slope_two + 2.0 * slope_three + slope_four)
```

```python
import jax
import jax.numpy as jnp
from jax import lax
from jax.experimental import pallas as pl
from jax.experimental.pallas import tpu as pltpu
from jax.sharding import PartitionSpec as P

NV = 5
CA = 8
AXIAL_MACH = 0.4
STEP = 0.3
F32 = jnp.float32
INTERPRET = False


def call(kernel, out_shape, *args):
    spec = pl.BlockSpec(memory_space=pltpu.VMEM)
    many = isinstance(out_shape, tuple)
    return pl.pallas_call(
        kernel,
        in_specs=[spec] * len(args),
        out_specs=(spec,) * len(out_shape) if many else spec,
        out_shape=out_shape,
        interpret=INTERPRET,
    )(*[pltpu.with_memory_space_constraint(a, pltpu.VMEM) for a in args])


def sds(*shape):
    return pltpu.VMEM(shape, F32)


def lanes():
    return lax.broadcasted_iota(jnp.int32, (8, 128), 1)


def subs():
    return lax.broadcasted_iota(jnp.int32, (8, 128), 0)


def is_even(axis):
    return lax.axis_index(axis) % 2 == 0


def radial_out(state, eddy, inner, outer):
    upper = subs() < 4
    even_rad = is_even("rad")
    for field in range(NV + 1):
        for pair in range(CA // 2):
            if field < NV:
                even, odd = state[field, 2 * pair], state[field, 2 * pair + 1]
            else:
                even, odd = eddy[2 * pair], eddy[2 * pair + 1]
            to_low = jnp.where(upper, even, pltpu.roll(odd, 4, 0))
            to_high = jnp.where(upper, pltpu.roll(even, 4, 0), odd)
            inner[field, pair] = jnp.where(even_rad, to_high, to_low)
            outer[field, pair] = jnp.where(even_rad, to_low, to_high)


def matrices(index, weight, out):
    side = lax.axis_index("ax")
    rows = lax.broadcasted_iota(jnp.int32, (128, 128), 0)
    for section in range(4):
        taps_at = index[side, section]
        weights = weight[side, section]
        weights = weights / jnp.sum(weights, axis=0, keepdims=True)
        total = jnp.zeros((128, 128), F32)
        for tap in range(4):
            total = total + jnp.where(rows == taps_at[tap : tap + 1], weights[tap : tap + 1], 0.0)
        out[section] = total


def send_edges(tiles, inner, outer, half):
    lane = lanes()
    first = jnp.zeros((8, 128), F32)
    last = jnp.zeros((8, 128), F32)
    for var in range(NV):
        for a in range(CA):
            k = var * CA + a
            x = tiles[var][a]
            first = jnp.where(lane == k, pltpu.roll(x, k, 1) if k else x, first)
            last = jnp.where(lane == k, pltpu.roll(x, k + 1, 1), last)
    even = is_even("circ")
    inner[pl.ds(8 * half, 8)] = jnp.where(even, last, first)
    outer[pl.ds(8 * half, 8)] = jnp.where(even, first, last)


def assemble(state, eddy, from_inner, from_outer, ext, eddy_ext, plane, west, east):
    upper = subs() < 4
    is_rotor = lax.axis_index("ax") == 1
    even_rad = is_even("rad")
    tiles = [[], []]
    for field in range(NV + 1):
        own_row, far_row = [], []
        for a in range(CA):
            pair = a // 2
            near, other = from_inner[field, pair], from_outer[field, pair]
            high = jnp.where(even_rad, near, other)
            low = jnp.where(even_rad, other, near)
            if a % 2 == 0:
                far = jnp.where(upper, high, pltpu.roll(low, 4, 0))
            else:
                far = jnp.where(upper, pltpu.roll(high, 4, 0), low)
            own = state[field, a] if field < NV else eddy[a]
            if field < NV:
                ext[field, a, 0:8] = own
                ext[field, a, 8:16] = far
            else:
                eddy_ext[a, 0:8] = own
                eddy_ext[a, 8:16] = far
            own_row.append(own)
            far_row.append(far)
        tiles[0].append(own_row)
        tiles[1].append(far_row)
    for half in range(2):
        for var in range(NV):
            plane[var, pl.ds(8 * half, 8)] = jnp.where(is_rotor, tiles[half][var][0], tiles[half][var][CA - 1])
        send_edges(tiles[half], west, east, half)


def section_body(last, first, refs):
    if last:
        field, base, acc_in, eddy, ghost_in, matrix, from_inner, from_outer, out = refs
    elif first:
        field, eddy, ghost_in, matrix, from_inner, from_outer, nxt, acc_out, plane, west, east = refs
        base = field
    else:
        field, base, acc_in, eddy, ghost_in, matrix, from_inner, from_outer, nxt, acc_out, plane, west, east = refs
    section = refs_section[0]
    lane, sub = lanes(), subs()
    even_circ = is_even("circ")
    is_rotor = lax.axis_index("ax") == 1
    rad = lax.axis_index("rad")
    count = lax.axis_size("rad")
    swirl = jnp.where(is_rotor, F32(-0.3), F32(0.2))
    halves = 1 if last else 2
    ghost = jnp.dot(
        ghost_in[...].reshape(NV * 8 * halves, 128),
        matrix[section],
        precision=lax.Precision.HIGHEST,
        preferred_element_type=F32,
    ).reshape(NV, 8 * halves, 128)
    inside = jnp.where(sub < 4, jnp.where(rad == count - 1, 0.0, 1.0), jnp.where(rad == 0, 0.0, 1.0)).astype(F32)
    step = (0.5 * STEP, 0.5 * STEP, STEP, 0.0)[section]
    gain = STEP / 6.0 * (1.0, 2.0, 2.0, 1.0)[section]
    x = [[[field[v, a, 0:8], field[v, a, 8:16]] for a in range(CA)] for v in range(NV)]
    zero = jnp.zeros((8, 128), F32)
    tiles = [[[None] * CA for _ in range(NV)] for _ in range(2)]
    for half in range(halves):
        near, other = from_inner[pl.ds(8 * half, 8)], from_outer[pl.ds(8 * half, 8)]
        west_msg = jnp.where(even_circ, other, near)
        east_msg = jnp.where(even_circ, near, other)
        for a in range(CA):
            e = eddy[a, pl.ds(8 * half, 8)]
            dc, dr, da, lap = [], [], [], []
            for v in range(NV):
                k = v * CA + a
                c = x[v][a][half]
                o = x[v][a][1 - half]
                cp = jnp.where(lane == 0, pltpu.roll(west_msg, (128 - k) % 128, 1) if k else west_msg, pltpu.roll(c, 1, 1))
                cn = jnp.where(lane == 127, pltpu.roll(east_msg, 127 - k, 1), pltpu.roll(c, 127, 1))
                up = pltpu.roll(jnp.where(sub == 0, o, c), 7, 0)
                dn = pltpu.roll(jnp.where(sub == 7, o, c), 1, 0)
                g = ghost[v, 8 * half : 8 * half + 8]
                lo = x[v][a - 1][half] if a > 0 else jnp.where(is_rotor, g, zero)
                hi = x[v][a + 1][half] if a < CA - 1 else jnp.where(is_rotor, zero, g)
                dc.append(cn - cp)
                dr.append(up - dn)
                da.append(hi - lo)
                lap.append((cn + cp) + (up + dn) + (hi + lo) - 6.0 * c)
            div = 0.5 * (dc[1] + dr[2] + da[3])
            flux = (div, 0.5 * dc[4], 0.5 * dr[4], 0.5 * da[4], div)
            for v in range(NV):
                slope = e * lap[v] - (0.5 * swirl) * dc[v] - (0.5 * AXIAL_MACH) * da[v] - flux[v]
                rows = pl.ds(8 * half, 8)
                if last:
                    out[v, a] = acc_in[v, a] + gain * slope
                    continue
                if half == 1:
                    slope = slope * inside
                u = base[v, a, rows] + step * slope
                nxt[v, a, rows] = u
                tiles[half][v][a] = u
                if half == 0:
                    acc_out[v, a] = (base[v, a, 0:8] if first else acc_in[v, a]) + gain * slope
    if last:
        return
    send_halves = 1 if section == 2 else 2
    for half in range(send_halves):
        for v in range(NV):
            plane[v, pl.ds(8 * half, 8)] = jnp.where(is_rotor, tiles[half][v][0], tiles[half][v][CA - 1])
        send_edges(tiles[half], west, east, half)


refs_section = [0]


def section_call(section, *args):
    last, first = section == 3, section == 0

    def kernel(*refs):
        refs_section[0] = section
        section_body(last, first, refs)

    if last:
        return call(kernel, jax.ShapeDtypeStruct((NV, CA, 8, 128), F32), *args)
    rows = 8 if section == 2 else 16
    shapes = (sds(NV, CA, 16, 128), sds(NV, CA, 8, 128), sds(NV, rows, 128), sds(rows, 128), sds(rows, 128))
    return call(kernel, shapes, *args)


SPECIAL = (0, 16, 31)


def inner_pairs(count):
    return [(i, i ^ 1) for i in range(count)]


def outer_pairs(count, wrap):
    pairs = [(i, i + 1 if i % 2 else i - 1) for i in range(count)]
    return [(i, j % count) for i, j in pairs if wrap or 0 <= j < count]


def facing(plane, offset):
    count = lax.axis_size("circ")
    pairs = [(2 * ((c + offset) % count), 2 * c + 1) for c in range(count)]
    pairs += [(j, i) for i, j in pairs]
    return lax.ppermute(plane, ("circ", "ax"), pairs)


def beside(inner, outer):
    count = lax.axis_size("circ")
    from_outer = lax.ppermute(outer, "circ", outer_pairs(count, True))
    from_inner = lax.ppermute(inner, "circ", inner_pairs(count))
    return from_inner, from_outer


def exchange(kind, place, plane, inner, outer):
    others = [o for o in range(lax.axis_size("circ")) if o not in SPECIAL]

    def special(o):
        return lambda plane, inner, outer: (facing(plane, o), *beside(inner, outer))

    def general(plane, inner, outer):
        sides = beside(inner, outer)
        ghost = lax.switch(place, [lambda p, o=o: facing(p, o) for o in others], plane)
        return (ghost, *sides)

    return lax.switch(kind, [special(o) for o in SPECIAL] + [general], plane, inner, outer)


def local(state, eddy, offsets, stencil_index, stencil_weight):
    index = jnp.transpose(stencil_index, (0, 1, 3, 2))
    weight = jnp.transpose(stencil_weight, (0, 1, 3, 2))
    count = lax.axis_size("rad")
    kind = jnp.where(offsets == 0, 0, jnp.where(offsets == 16, 1, jnp.where(offsets == 31, 2, 3)))
    place = offsets - (offsets > 0).astype(jnp.int32) - (offsets > 16).astype(jnp.int32)
    message = sds(NV + 1, CA // 2, 8, 128)
    inner, outer = call(radial_out, (message, message), state, eddy)
    from_outer = lax.ppermute(outer, "rad", outer_pairs(count, False))
    from_inner = lax.ppermute(inner, "rad", inner_pairs(count))
    matrix = call(matrices, sds(4, 128, 128), index, weight)
    ext, eddy_ext, plane, west, east = call(
        assemble,
        (sds(NV, CA, 16, 128), sds(CA, 16, 128), sds(NV, 16, 128), sds(16, 128), sds(16, 128)),
        state, eddy, from_inner, from_outer,
    )
    ghost, fw, fe = exchange(kind[0], place[0], plane, west, east)
    field, acc, plane, west, east = section_call(0, ext, eddy_ext, ghost, matrix, fw, fe)
    for section in (1, 2):
        ghost, fw, fe = exchange(kind[section], place[section], plane, west, east)
        field, acc, plane, west, east = section_call(section, field, ext, acc, eddy_ext, ghost, matrix, fw, fe)
    ghost, fw, fe = exchange(kind[3], place[3], plane, west, east)
    return section_call(3, field, ext, acc, eddy_ext, ghost, matrix, fw, fe)


def solution(mesh):
    return jax.shard_map(
        local,
        mesh=mesh,
        in_specs=(P(None, "ax", "rad", "circ"), P("ax", "rad", "circ"), P(), P(), P()),
        out_specs=P(None, "ax", "rad", "circ"),
        check_vma=False,
    )
```

```python
import jax
import jax.numpy as jnp
from jax import lax
from jax.experimental import pallas as pl
from jax.experimental.pallas import tpu as pltpu
from jax.sharding import PartitionSpec as P

NV = 5
CA = 8
AXIAL_MACH = 0.4
STEP = 0.3
F32 = jnp.float32
INTERPRET = False


def call(kernel, out_shape, *args):
    spec = pl.BlockSpec(memory_space=pltpu.VMEM)
    many = isinstance(out_shape, tuple)
    return pl.pallas_call(
        kernel,
        in_specs=[spec] * len(args),
        out_specs=(spec,) * len(out_shape) if many else spec,
        out_shape=out_shape,
        interpret=INTERPRET,
    )(*[pltpu.with_memory_space_constraint(a, pltpu.VMEM) for a in args])


def sds(*shape):
    return pltpu.VMEM(shape, F32)


def lanes():
    return lax.broadcasted_iota(jnp.int32, (8, 128), 1)


def subs():
    return lax.broadcasted_iota(jnp.int32, (8, 128), 0)


def is_even(axis):
    return lax.axis_index(axis) % 2 == 0


def radial_out(state, eddy, inner, outer):
    upper = subs() < 4
    even_rad = is_even("rad")
    for field in range(NV + 1):
        for pair in range(CA // 2):
            if field < NV:
                even, odd = state[field, 2 * pair], state[field, 2 * pair + 1]
            else:
                even, odd = eddy[2 * pair], eddy[2 * pair + 1]
            to_low = jnp.where(upper, even, pltpu.roll(odd, 4, 0))
            to_high = jnp.where(upper, pltpu.roll(even, 4, 0), odd)
            inner[field, pair] = jnp.where(even_rad, to_high, to_low)
            outer[field, pair] = jnp.where(even_rad, to_low, to_high)


def matrices(index, weight, out):
    side = lax.axis_index("ax")
    rows = lax.broadcasted_iota(jnp.int32, (128, 128), 0)
    for section in range(4):
        taps_at = index[side, section]
        weights = weight[side, section]
        weights = weights / jnp.sum(weights, axis=0, keepdims=True)
        total = jnp.zeros((128, 128), F32)
        for tap in range(4):
            total = total + jnp.where(rows == taps_at[tap : tap + 1], weights[tap : tap + 1], 0.0)
        out[section] = total


def edges_kernel(section):
    def kernel(field, eddy, received, matrix, face, inner, outer):
        lane = lanes()
        even = is_even("circ")
        ghost = interpolated(received, matrix, section)
        face[...] = ghost
        for half in range(2):
            rows = slice(8 * half, 8 * half + 8)
            first = jnp.zeros((8, 128), F32)
            last = jnp.zeros((8, 128), F32)
            for var in range(NV):
                for a in range(CA):
                    k = var * CA + a
                    x = field[var, a, rows]
                    first = place(first, x, 0, k)
                    first = place(first, x, 1, 40 + k)
                    last = place(last, x, 127, k)
                    last = place(last, x, 126, 40 + k)
            for a in range(CA):
                first = place(first, eddy[a, rows], 0, 80 + a)
                last = place(last, eddy[a, rows], 127, 80 + a)
            for var in range(NV):
                for a in (0, CA - 1):
                    k = 88 + var * CA + a
                    first = place(first, ghost[var, rows], 0, k)
                    last = place(last, ghost[var, rows], 127, k)
            inner[rows] = jnp.where(even, last, first)
            outer[rows] = jnp.where(even, first, last)

    return kernel


def turn(x, amount, axis=1):
    amount %= x.shape[axis]
    return pltpu.roll(x, amount, axis) if amount else x


def place(tile, x, source, target):
    return jnp.where(lanes() == target, turn(x, target - source), tile)


def interpolated(received, matrix, section):
    rows = received.shape[1]
    flat = received[...].reshape(NV * rows, 128)
    ghost = jnp.dot(flat, matrix[section], precision=lax.Precision.HIGHEST, preferred_element_type=F32)
    return ghost.reshape(NV, rows, 128)


def side_column(tile, other, own, west, is_rotor, swirl):
    lane, sub = lanes(), subs()
    far = turn(tile, -40)
    low_c, high_c = (far, own) if west else (own, far)
    up = turn(jnp.where(sub == 0, other, tile), 7, 0)
    down = turn(jnp.where(sub == 7, other, tile), 1, 0)
    ghost = turn(tile, -88)
    low = jnp.where(lane % CA == 0, jnp.where(is_rotor, ghost, 0.0), turn(tile, 1))
    high = jnp.where(lane % CA == CA - 1, jnp.where(is_rotor, 0.0, ghost), turn(tile, -1))
    part = jnp.where(lane < CA, turn(tile, -80), 0.0)
    e = part
    for var in range(1, NV):
        e = e + turn(part, CA * var)
    dc, dr, da = high_c - low_c, up - down, high - low
    lap = (high_c + low_c) + (up + down) + (high + low) - 6.0 * tile
    div = turn(dc, -CA) + turn(dr, -2 * CA) + turn(da, -3 * CA)
    flux = turn(div, 4 * CA)
    flux = jnp.where(lane < 4 * CA, turn(da, -CA), flux)
    flux = jnp.where(lane < 3 * CA, turn(dr, -2 * CA), flux)
    flux = jnp.where(lane < 2 * CA, turn(dc, -3 * CA), flux)
    flux = jnp.where(lane < CA, div, flux)
    return e * lap - (0.5 * swirl) * dc - (0.5 * AXIAL_MACH) * da - 0.5 * flux


def assemble(state, eddy, from_inner, from_outer, ext, eddy_ext, plane):
    upper = subs() < 4
    is_rotor = lax.axis_index("ax") == 1
    even_rad = is_even("rad")
    tiles = [[], []]
    for field in range(NV + 1):
        own_row, far_row = [], []
        for a in range(CA):
            pair = a // 2
            near, other = from_inner[field, pair], from_outer[field, pair]
            high = jnp.where(even_rad, near, other)
            low = jnp.where(even_rad, other, near)
            if a % 2 == 0:
                far = jnp.where(upper, high, pltpu.roll(low, 4, 0))
            else:
                far = jnp.where(upper, pltpu.roll(high, 4, 0), low)
            own = state[field, a] if field < NV else eddy[a]
            if field < NV:
                ext[field, a, 0:8] = own
                ext[field, a, 8:16] = far
            else:
                eddy_ext[a, 0:8] = own
                eddy_ext[a, 8:16] = far
            own_row.append(own)
            far_row.append(far)
        tiles[0].append(own_row)
        tiles[1].append(far_row)
    for half in range(2):
        for var in range(NV):
            plane[var, pl.ds(8 * half, 8)] = jnp.where(is_rotor, tiles[half][var][0], tiles[half][var][CA - 1])


def section_kernel(section):
    last, first, paired = section == 3, section == 0, section % 2 == 0

    def kernel(*refs):
        refs = list(refs)
        field = refs.pop(0)
        base = field if first else refs.pop(0)
        acc_in = None if first else refs.pop(0)
        eddy = refs.pop(0)
        if paired:
            face, own_inner, own_outer, from_inner, from_outer = refs[:5]
            refs = refs[5:]
            start_inner, start_outer = (from_inner, from_outer) if first else (refs.pop(0), refs.pop(0))
            ghost = face[...]
        else:
            received, matrix, sides_in = refs[:3]
            refs = refs[3:]
            ghost = interpolated(received, matrix, section)
        if last:
            (out,) = refs
        elif paired:
            nxt, acc_out, plane, sides = refs
        else:
            nxt, acc_out, plane = refs
        lane, sub = lanes(), subs()
        even = is_even("circ")
        is_rotor = lax.axis_index("ax") == 1
        rad = lax.axis_index("rad")
        count = lax.axis_size("rad")
        swirl = jnp.where(is_rotor, F32(-0.3), F32(0.2))
        inside = jnp.where(sub < 4, jnp.where(rad == count - 1, 0.0, 1.0), jnp.where(rad == 0, 0.0, 1.0)).astype(F32)
        step = (0.5 * STEP, 0.5 * STEP, STEP, 0.0)[section]
        gain = STEP / 6.0 * (1.0, 2.0, 2.0, 1.0)[section]
        send_halves = {0: 2, 1: 2, 2: 1, 3: 0}[section]
        zero = jnp.zeros((8, 128), F32)

        def tile(v, a, half):
            return field[v, a, 8 * half : 8 * half + 8]

        def pick(near, beyond, half):
            rows = slice(8 * half, 8 * half + 8)
            x, y = near[rows], beyond[rows]
            return jnp.where(even, y, x), jnp.where(even, x, y)

        for half in range(1 if last else 2):
            rows = slice(8 * half, 8 * half + 8)
            if paired:
                west, east = pick(from_inner, from_outer, half)
            else:
                west, east = sides_in[0, rows], sides_in[1, rows]
            if paired and half < send_halves:
                other_west, other_east = pick(from_inner, from_outer, 1 - half)
                own_last, own_first = pick(own_outer, own_inner, half)
                base_west, base_east = pick(start_inner, start_outer, half)
                for n, (beside, beyond, own, old) in enumerate(
                    ((west, other_west, own_first, base_west), (east, other_east, own_last, base_east))
                ):
                    slope = side_column(beside, beyond, own, n == 0, is_rotor, swirl)
                    if half == 1:
                        slope = slope * inside
                    sides[n, rows] = old + step * slope
            for a in range(CA):
                e = eddy[a, rows]
                dc, dr, da, lap = [], [], [], []
                for v in range(NV):
                    k = v * CA + a
                    c = tile(v, a, half)
                    o = tile(v, a, 1 - half)
                    cp = jnp.where(lane == 0, turn(west, -k), turn(c, 1))
                    cn = jnp.where(lane == 127, turn(east, 127 - k), turn(c, -1))
                    up = turn(jnp.where(sub == 0, o, c), 7, 0)
                    dn = turn(jnp.where(sub == 7, o, c), 1, 0)
                    g = ghost[v, rows]
                    lo = tile(v, a - 1, half) if a > 0 else jnp.where(is_rotor, g, zero)
                    hi = tile(v, a + 1, half) if a < CA - 1 else jnp.where(is_rotor, zero, g)
                    dc.append(cn - cp)
                    dr.append(up - dn)
                    da.append(hi - lo)
                    lap.append((cn + cp) + (up + dn) + (hi + lo) - 6.0 * c)
                div = 0.5 * (dc[1] + dr[2] + da[3])
                flux = (div, 0.5 * dc[4], 0.5 * dr[4], 0.5 * da[4], div)
                for v in range(NV):
                    slope = e * lap[v] - (0.5 * swirl) * dc[v] - (0.5 * AXIAL_MACH) * da[v] - flux[v]
                    if last:
                        out[v, a] = acc_in[v, a] + gain * slope
                        continue
                    if half == 1:
                        slope = slope * inside
                    u = base[v, a, rows] + step * slope
                    nxt[v, a, rows] = u
                    if half == 0:
                        acc_out[v, a] = (base[v, a, 0:8] if first else acc_in[v, a]) + gain * slope
            if half < send_halves:
                for v in range(NV):
                    plane[v, rows] = jnp.where(is_rotor, nxt[v, 0, rows], nxt[v, CA - 1, rows])

    return kernel


def section_call(section, *args):
    if section == 3:
        return call(section_kernel(3), jax.ShapeDtypeStruct((NV, CA, 8, 128), F32), *args)
    rows = 8 if section == 2 else 16
    shapes = (sds(NV, CA, 16, 128), sds(NV, CA, 8, 128), sds(NV, rows, 128))
    if section != 1:
        shapes += (sds(2, rows, 128),)
    return call(section_kernel(section), shapes, *args)


def inner_pairs(count):
    return [(i, i ^ 1) for i in range(count)]


def outer_pairs(count, wrap):
    pairs = [(i, i + 1 if i % 2 else i - 1) for i in range(count)]
    return [(i, j % count) for i, j in pairs if wrap or 0 <= j < count]


def same(source, out):
    out[...] = source[...]


def facing(plane, offset):
    count = lax.axis_size("circ")
    pairs = [(2 * ((c + offset) % count), 2 * c + 1) for c in range(count)]
    pairs += [(j, i) for i, j in pairs]
    ghost = lax.ppermute(plane, ("circ", "ax"), pairs)
    return call(same, sds(*ghost.shape), ghost)


def ghost_of(offset, plane):
    count = lax.axis_size("circ")
    return lax.switch(offset, [lambda p, o=o: facing(p, o) for o in range(count)], plane)


def beside(section, field, eddy, received, matrix):
    count = lax.axis_size("circ")
    shapes = (sds(NV, 16, 128), sds(16, 128), sds(16, 128))
    face, inner, outer = call(edges_kernel(section), shapes, field, eddy, received, matrix)
    from_outer = lax.ppermute(outer, "circ", outer_pairs(count, True))
    from_inner = lax.ppermute(inner, "circ", inner_pairs(count))
    return face, inner, outer, from_inner, from_outer


def local(state, eddy, offsets, stencil_index, stencil_weight):
    index = jnp.transpose(stencil_index, (0, 1, 3, 2))
    weight = jnp.transpose(stencil_weight, (0, 1, 3, 2))
    count = lax.axis_size("rad")
    message = sds(NV + 1, CA // 2, 8, 128)
    inner, outer = call(radial_out, (message, message), state, eddy)
    from_outer = lax.ppermute(outer, "rad", outer_pairs(count, False))
    from_inner = lax.ppermute(inner, "rad", inner_pairs(count))
    matrix = call(matrices, sds(4, 128, 128), index, weight)
    places = [offsets[section] for section in range(4)]
    from_inner, from_outer, matrix, *places = lax.optimization_barrier((from_inner, from_outer, matrix, *places))
    ext, eddy_ext, plane = call(
        assemble,
        (sds(NV, CA, 16, 128), sds(CA, 16, 128), sds(NV, 16, 128)),
        state, eddy, from_inner, from_outer,
    )
    received = ghost_of(places[0], plane)
    edges = beside(0, ext, eddy_ext, received, matrix)
    field, acc, plane, sides = section_call(0, ext, eddy_ext, *edges)
    received = ghost_of(places[1], plane)
    field, acc, plane = section_call(1, field, ext, acc, eddy_ext, received, matrix, sides)
    received = ghost_of(places[2], plane)
    later = beside(2, field, eddy_ext, received, matrix)
    field, acc, plane, sides = section_call(2, field, ext, acc, eddy_ext, *later, *edges[3:])
    received = ghost_of(places[3], plane)
    return section_call(3, field, ext, acc, eddy_ext, received, matrix, sides)


def solution(mesh):
    return jax.shard_map(
        local,
        mesh=mesh,
        in_specs=(P(None, "ax", "rad", "circ"), P("ax", "rad", "circ"), P(), P(), P()),
        out_specs=P(None, "ax", "rad", "circ"),
        check_vma=False,
    )
```

```python
import jax
import jax.numpy as jnp
from jax import lax
from jax.experimental import pallas as pl
from jax.experimental.pallas import tpu as pltpu
from jax.sharding import PartitionSpec as P

NV = 5
CA = 8
AXIAL_MACH = 0.4
STEP = 0.3
F32 = jnp.float32
INTERPRET = False


def call(kernel, out_shape, *args):
    spec = pl.BlockSpec(memory_space=pltpu.VMEM)
    many = isinstance(out_shape, tuple)
    return pl.pallas_call(
        kernel,
        in_specs=[spec] * len(args),
        out_specs=(spec,) * len(out_shape) if many else spec,
        out_shape=out_shape,
        interpret=INTERPRET,
    )(*[pltpu.with_memory_space_constraint(a, pltpu.VMEM) for a in args])


def sds(*shape):
    return pltpu.VMEM(shape, F32)


def lanes():
    return lax.broadcasted_iota(jnp.int32, (8, 128), 1)


def subs():
    return lax.broadcasted_iota(jnp.int32, (8, 128), 0)


def is_even(axis):
    return lax.axis_index(axis) % 2 == 0


def radial_out(state_in, eddy_in, inner, outer, state, eddy, done):
    copies = [
        pltpu.make_async_copy(state_in, state, done.at[0]),
        pltpu.make_async_copy(eddy_in, eddy, done.at[1]),
    ]
    for copy in copies:
        copy.start()
    for copy in copies:
        copy.wait()
    upper = subs() < 4
    even_rad = is_even("rad")
    for field in range(NV + 1):
        for pair in range(CA // 2):
            if field < NV:
                even, odd = state[field, 2 * pair], state[field, 2 * pair + 1]
            else:
                even, odd = eddy[2 * pair], eddy[2 * pair + 1]
            to_low = jnp.where(upper, even, pltpu.roll(odd, 4, 0))
            to_high = jnp.where(upper, pltpu.roll(even, 4, 0), odd)
            inner[field, pair] = jnp.where(even_rad, to_high, to_low)
            outer[field, pair] = jnp.where(even_rad, to_low, to_high)


def matrices(index, weight, out):
    side = lax.axis_index("ax")
    rows = lax.broadcasted_iota(jnp.int32, (128, 128), 0)
    for section in range(4):
        taps_at = index[side, section]
        weights = weight[side, section]
        weights = weights / jnp.sum(weights, axis=0, keepdims=True)
        total = jnp.zeros((128, 128), F32)
        for tap in range(4):
            total = total + jnp.where(rows == taps_at[tap : tap + 1], weights[tap : tap + 1], 0.0)
        out[section] = total


def edges_kernel(section):
    def kernel(field, eddy, received, matrix, face, outer, inner):
        lane = lanes()
        even = is_even("circ")
        ghost = interpolated(received, matrix, section)
        face[...] = ghost
        for half in range(2):
            rows = slice(8 * half, 8 * half + 8)
            first = jnp.zeros((8, 128), F32)
            last = jnp.zeros((8, 128), F32)
            for var in range(NV):
                for a in range(CA):
                    k = var * CA + a
                    x = field[var, a, rows]
                    first = place(first, x, 0, k)
                    first = place(first, x, 1, 40 + k)
                    last = place(last, x, 127, k)
                    last = place(last, x, 126, 40 + k)
            for a in range(CA):
                first = place(first, eddy[a, rows], 0, 80 + a)
                last = place(last, eddy[a, rows], 127, 80 + a)
            for var in range(NV):
                for a in (0, CA - 1):
                    k = 88 + var * CA + a
                    first = place(first, ghost_tile(ghost, section, var, half), 0, k)
                    last = place(last, ghost_tile(ghost, section, var, half), 127, k)
            inner[rows] = jnp.where(even, last, first)
            outer[rows] = jnp.where(even, first, last)

    return kernel


def turn(x, amount, axis=1):
    amount %= x.shape[axis]
    return pltpu.roll(x, amount, axis) if amount else x


def place(tile, x, source, target):
    return jnp.where(lanes() == target, turn(x, target - source), tile)


def interpolated(received, matrix, section):
    count = received.shape[0]
    flat = received[...].reshape(count * 8, 128)
    ghost = jnp.dot(flat, matrix[section], precision=lax.Precision.HIGHEST, preferred_element_type=F32)
    return ghost.reshape(count, 8, 128)


SHARED = (1, 2, 4)


def plane_tiles(section):
    return NV if section == 3 else NV + -(-NV // SHARED[section])


def write_plane(plane, section, own, halo):
    for v in range(NV):
        plane[v] = own[v]
    if section == 3:
        return
    shared = SHARED[section]
    shift, need, sub = 8 // shared, 3 - section, subs()
    for start in range(0, NV, shared):
        tile = halo[start]
        for v in range(start + 1, min(start + shared, NV)):
            row = (sub + 8 - shift * (v - start)) % 8
            tile = jnp.where((row < need) | (row >= 8 - need), turn(halo[v], shift * (v - start), 0), tile)
        plane[NV + start // shared] = tile


def ghost_tile(ghost, section, v, half):
    if half == 0:
        return ghost[v]
    shared = SHARED[section]
    return turn(ghost[NV + v // shared], -(8 // shared) * (v % shared), 0)


def side_column(tile, other, own, west, is_rotor, swirl):
    lane, sub = lanes(), subs()
    far = turn(tile, -40)
    low_c, high_c = (far, own) if west else (own, far)
    up = turn(jnp.where(sub == 0, other, tile), 7, 0)
    down = turn(jnp.where(sub == 7, other, tile), 1, 0)
    ghost = turn(tile, -88)
    low = jnp.where(lane % CA == 0, jnp.where(is_rotor, ghost, 0.0), turn(tile, 1))
    high = jnp.where(lane % CA == CA - 1, jnp.where(is_rotor, 0.0, ghost), turn(tile, -1))
    part = jnp.where(lane < CA, turn(tile, -80), 0.0)
    e = part
    for var in range(1, NV):
        e = e + turn(part, CA * var)
    dc, dr, da = high_c - low_c, up - down, high - low
    lap = (high_c + low_c) + (up + down) + (high + low) - 6.0 * tile
    div = turn(dc, -CA) + turn(dr, -2 * CA) + turn(da, -3 * CA)
    flux = turn(div, 4 * CA)
    flux = jnp.where(lane < 4 * CA, turn(da, -CA), flux)
    flux = jnp.where(lane < 3 * CA, turn(dr, -2 * CA), flux)
    flux = jnp.where(lane < 2 * CA, turn(dc, -3 * CA), flux)
    flux = jnp.where(lane < CA, div, flux)
    return e * lap - (0.5 * swirl) * dc - (0.5 * AXIAL_MACH) * da - 0.5 * flux


def assemble(state, eddy, from_outer, from_inner, ext, eddy_ext, plane):
    upper = subs() < 4
    is_rotor = lax.axis_index("ax") == 1
    even_rad = is_even("rad")
    tiles = [[], []]
    for field in range(NV + 1):
        own_row, far_row = [], []
        for a in range(CA):
            pair = a // 2
            near, other = from_inner[field, pair], from_outer[field, pair]
            high = jnp.where(even_rad, near, other)
            low = jnp.where(even_rad, other, near)
            if a % 2 == 0:
                far = jnp.where(upper, high, pltpu.roll(low, 4, 0))
            else:
                far = jnp.where(upper, pltpu.roll(high, 4, 0), low)
            own = state[field, a] if field < NV else eddy[a]
            if field < NV:
                ext[field, a, 0:8] = own
                ext[field, a, 8:16] = far
            else:
                eddy_ext[a, 0:8] = own
                eddy_ext[a, 8:16] = far
            own_row.append(own)
            far_row.append(far)
        tiles[0].append(own_row)
        tiles[1].append(far_row)
    planes = [[jnp.where(is_rotor, row[0], row[CA - 1]) for row in tiles[half]] for half in range(2)]
    write_plane(plane, 0, *planes)


def section_kernel(section):
    last, first, paired = section == 3, section == 0, section % 2 == 0

    def kernel(*refs):
        refs = list(refs)
        field = refs.pop(0)
        base = field if first else refs.pop(0)
        acc_in = None if first else refs.pop(0)
        eddy = refs.pop(0)
        if paired:
            face, own_outer, own_inner, from_outer, from_inner = refs[:5]
            refs = refs[5:]
            start_outer, start_inner = (from_outer, from_inner) if first else (refs.pop(0), refs.pop(0))
            ghost = face[...]
        else:
            received, matrix, sides_in = refs[:3]
            refs = refs[3:]
            ghost = interpolated(received, matrix, section)
        if last:
            (out,) = refs
        elif paired:
            nxt, acc_out, plane, sides = refs
        else:
            nxt, acc_out, plane = refs
        lane, sub = lanes(), subs()
        even = is_even("circ")
        is_rotor = lax.axis_index("ax") == 1
        rad = lax.axis_index("rad")
        count = lax.axis_size("rad")
        swirl = jnp.where(is_rotor, F32(-0.3), F32(0.2))
        inside = jnp.where(sub < 4, jnp.where(rad == count - 1, 0.0, 1.0), jnp.where(rad == 0, 0.0, 1.0)).astype(F32)
        step = (0.5 * STEP, 0.5 * STEP, STEP, 0.0)[section]
        gain = STEP / 6.0 * (1.0, 2.0, 2.0, 1.0)[section]
        send_halves = {0: 2, 1: 2, 2: 1, 3: 0}[section]
        zero = jnp.zeros((8, 128), F32)

        def tile(v, a, half):
            return field[v, a, 8 * half : 8 * half + 8]

        def pick(near, beyond, half):
            rows = slice(8 * half, 8 * half + 8)
            x, y = near[rows], beyond[rows]
            return jnp.where(even, y, x), jnp.where(even, x, y)

        for half in range(1 if last else 2):
            rows = slice(8 * half, 8 * half + 8)
            if paired:
                west, east = pick(from_inner, from_outer, half)
            else:
                west, east = sides_in[0, rows], sides_in[1, rows]
            if paired and half < send_halves:
                other_west, other_east = pick(from_inner, from_outer, 1 - half)
                own_last, own_first = pick(own_outer, own_inner, half)
                base_west, base_east = pick(start_inner, start_outer, half)
                for n, (beside, beyond, own, old) in enumerate(
                    ((west, other_west, own_first, base_west), (east, other_east, own_last, base_east))
                ):
                    slope = side_column(beside, beyond, own, n == 0, is_rotor, swirl)
                    if half == 1:
                        slope = slope * inside
                    sides[n, rows] = old + step * slope
            for a in range(CA):
                e = eddy[a, rows]
                dc, dr, da, lap = [], [], [], []
                for v in range(NV):
                    k = v * CA + a
                    c = tile(v, a, half)
                    o = tile(v, a, 1 - half)
                    cp = jnp.where(lane == 0, turn(west, -k), turn(c, 1))
                    cn = jnp.where(lane == 127, turn(east, 127 - k), turn(c, -1))
                    up = turn(jnp.where(sub == 0, o, c), 7, 0)
                    dn = turn(jnp.where(sub == 7, o, c), 1, 0)
                    g = ghost_tile(ghost, section, v, half)
                    lo = tile(v, a - 1, half) if a > 0 else jnp.where(is_rotor, g, zero)
                    hi = tile(v, a + 1, half) if a < CA - 1 else jnp.where(is_rotor, zero, g)
                    dc.append(cn - cp)
                    dr.append(up - dn)
                    da.append(hi - lo)
                    lap.append((cn + cp) + (up + dn) + (hi + lo) - 6.0 * c)
                div = 0.5 * (dc[1] + dr[2] + da[3])
                flux = (div, 0.5 * dc[4], 0.5 * dr[4], 0.5 * da[4], div)
                for v in range(NV):
                    slope = e * lap[v] - (0.5 * swirl) * dc[v] - (0.5 * AXIAL_MACH) * da[v] - flux[v]
                    if last:
                        out[v, a] = acc_in[v, a] + gain * slope
                        continue
                    if half == 1:
                        slope = slope * inside
                    u = base[v, a, rows] + step * slope
                    nxt[v, a, rows] = u
                    if half == 0:
                        acc_out[v, a] = (base[v, a, 0:8] if first else acc_in[v, a]) + gain * slope
        if not last:
            planes = [
                [jnp.where(is_rotor, nxt[v, 0, 8 * h : 8 * h + 8], nxt[v, CA - 1, 8 * h : 8 * h + 8]) for v in range(NV)]
                for h in range(2)
            ]
            write_plane(plane, section + 1, *planes)

    return kernel


def section_call(section, *args):
    if section == 3:
        return call(section_kernel(3), jax.ShapeDtypeStruct((NV, CA, 8, 128), F32), *args)
    rows = 8 if section == 2 else 16
    shapes = (sds(NV, CA, 16, 128), sds(NV, CA, 8, 128), sds(plane_tiles(section + 1), 8, 128))
    if section != 1:
        shapes += (sds(2, rows, 128),)
    return call(section_kernel(section), shapes, *args)


def inner_pairs(count):
    return [(i, i ^ 1) for i in range(count)]


def outer_pairs(count, wrap):
    pairs = [(i, i + 1 if i % 2 else i - 1) for i in range(count)]
    return [(i, j % count) for i, j in pairs if wrap or 0 <= j < count]


def same(source, out):
    out[...] = source[...]


def facing(plane, offset):
    count = lax.axis_size("circ")
    pairs = [(2 * ((c + offset) % count), 2 * c + 1) for c in range(count)]
    pairs += [(j, i) for i, j in pairs]
    ghost = lax.ppermute(plane, ("circ", "ax"), pairs)
    return call(same, sds(*ghost.shape), ghost)


def ghost_of(offset, plane):
    count = lax.axis_size("circ")
    return lax.switch(offset, [lambda p, o=o: facing(p, o) for o in range(count)], plane)


def beside(section, field, eddy, received, matrix):
    count = lax.axis_size("circ")
    shapes = (sds(plane_tiles(section), 8, 128), sds(16, 128), sds(16, 128))
    face, outer, inner = call(edges_kernel(section), shapes, field, eddy, received, matrix)
    from_outer = lax.ppermute(outer, "circ", outer_pairs(count, True))
    from_inner = lax.ppermute(inner, "circ", inner_pairs(count))
    return face, outer, inner, from_outer, from_inner


def local(state, eddy, offsets, stencil_index, stencil_weight):
    index = jnp.transpose(stencil_index, (0, 1, 3, 2))
    weight = jnp.transpose(stencil_weight, (0, 1, 3, 2))
    count = lax.axis_size("rad")
    message = sds(NV + 1, CA // 2, 8, 128)
    vmem = pl.BlockSpec(memory_space=pltpu.VMEM)
    inner, outer, own_state, own_eddy = pl.pallas_call(
        radial_out,
        in_specs=[pl.BlockSpec(memory_space=pl.ANY)] * 2,
        out_specs=(vmem,) * 4,
        out_shape=(message, message, sds(*state.shape), sds(*eddy.shape)),
        scratch_shapes=[pltpu.SemaphoreType.DMA((2,))],
        interpret=INTERPRET,
    )(state, eddy)
    from_outer = lax.ppermute(outer, "rad", outer_pairs(count, False))
    from_inner = lax.ppermute(inner, "rad", inner_pairs(count))
    matrix = call(matrices, sds(4, 128, 128), index, weight)
    places = [offsets[section] for section in range(4)]
    from_outer, from_inner, matrix, *places = lax.optimization_barrier((from_outer, from_inner, matrix, *places))
    ext, eddy_ext, plane = call(
        assemble,
        (sds(NV, CA, 16, 128), sds(CA, 16, 128), sds(plane_tiles(0), 8, 128)),
        own_state, own_eddy, from_outer, from_inner,
    )
    received = ghost_of(places[0], plane)
    edges = beside(0, ext, eddy_ext, received, matrix)
    field, acc, plane, sides = section_call(0, ext, eddy_ext, *edges)
    received = ghost_of(places[1], plane)
    field, acc, plane = section_call(1, field, ext, acc, eddy_ext, received, matrix, sides)
    received = ghost_of(places[2], plane)
    later = beside(2, field, eddy_ext, received, matrix)
    field, acc, plane, sides = section_call(2, field, ext, acc, eddy_ext, *later, *edges[3:])
    received = ghost_of(places[3], plane)
    return section_call(3, field, ext, acc, eddy_ext, received, matrix, sides)


def solution(mesh):
    return jax.shard_map(
        local,
        mesh=mesh,
        in_specs=(P(None, "ax", "rad", "circ"), P("ax", "rad", "circ"), P(), P(), P()),
        out_specs=P(None, "ax", "rad", "circ"),
        check_vma=False,
    )
```

```python
import jax
import jax.numpy as jnp
from jax import lax
from jax.experimental import pallas as pl
from jax.experimental.pallas import tpu as pltpu
from jax.sharding import PartitionSpec as P

NV = 5
CA = 8
AXIAL_MACH = 0.4
STEP = 0.3
F32 = jnp.float32
INTERPRET = False


def call(kernel, out_shape, *args):
    spec = pl.BlockSpec(memory_space=pltpu.VMEM)
    many = isinstance(out_shape, tuple)
    return pl.pallas_call(
        kernel,
        in_specs=[spec] * len(args),
        out_specs=(spec,) * len(out_shape) if many else spec,
        out_shape=out_shape,
        interpret=INTERPRET,
    )(*[pltpu.with_memory_space_constraint(a, pltpu.VMEM) for a in args])


def sds(*shape):
    return pltpu.VMEM(shape, F32)


def lanes():
    return lax.broadcasted_iota(jnp.int32, (8, 128), 1)


def subs():
    return lax.broadcasted_iota(jnp.int32, (8, 128), 0)


def is_even(axis):
    return lax.axis_index(axis) % 2 == 0


def radial_out(state_in, eddy_in, inner, outer, state, eddy, done):
    copies = [
        pltpu.make_async_copy(state_in, state, done.at[0]),
        pltpu.make_async_copy(eddy_in, eddy, done.at[1]),
    ]
    for copy in copies:
        copy.start()
    for copy in copies:
        copy.wait()
    upper = subs() < 4
    even_rad = is_even("rad")
    for field in range(NV + 1):
        for pair in range(CA // 2):
            if field < NV:
                even, odd = state[field, 2 * pair], state[field, 2 * pair + 1]
            else:
                even, odd = eddy[2 * pair], eddy[2 * pair + 1]
            to_low = jnp.where(upper, even, pltpu.roll(odd, 4, 0))
            to_high = jnp.where(upper, pltpu.roll(even, 4, 0), odd)
            inner[field, pair] = jnp.where(even_rad, to_high, to_low)
            outer[field, pair] = jnp.where(even_rad, to_low, to_high)


def matrices(index, weight, out):
    side = lax.axis_index("ax")
    rows = lax.broadcasted_iota(jnp.int32, (128, 128), 0)
    for section in range(4):
        taps_at = index[side, section]
        weights = weight[side, section]
        weights = weights / jnp.sum(weights, axis=0, keepdims=True)
        total = jnp.zeros((128, 128), F32)
        for tap in range(4):
            total = total + jnp.where(rows == taps_at[tap : tap + 1], weights[tap : tap + 1], 0.0)
        out[section] = total


def edges_kernel(section):
    def kernel(field, eddy, received, matrix, face, outer, inner):
        lane = lanes()
        even = is_even("circ")
        ghost = interpolated(received, matrix, section)
        face[...] = ghost
        for half in range(2):
            rows = slice(8 * half, 8 * half + 8)
            first = jnp.zeros((8, 128), F32)
            last = jnp.zeros((8, 128), F32)
            for var in range(NV):
                for a in range(CA):
                    k = var * CA + a
                    x = field[var, a, rows]
                    first = place(first, x, 0, k)
                    first = place(first, x, 1, 40 + k)
                    last = place(last, x, 127, k)
                    last = place(last, x, 126, 40 + k)
            for a in range(CA):
                first = place(first, eddy[a, rows], 0, 80 + a)
                last = place(last, eddy[a, rows], 127, 80 + a)
            for var in range(NV):
                for a in (0, CA - 1):
                    k = 88 + var * CA + a
                    first = place(first, ghost_tile(ghost, section, var, half), 0, k)
                    last = place(last, ghost_tile(ghost, section, var, half), 127, k)
            inner[rows] = jnp.where(even, last, first)
            outer[rows] = jnp.where(even, first, last)

    return kernel


def turn(x, amount, axis=1):
    amount %= x.shape[axis]
    return pltpu.roll(x, amount, axis) if amount else x


def place(tile, x, source, target):
    return jnp.where(lanes() == target, turn(x, target - source), tile)


def interpolated(received, matrix, section):
    count = received.shape[0]
    flat = received[...].reshape(count * 8, 128)
    ghost = jnp.dot(flat, matrix[section], precision=lax.Precision.HIGHEST, preferred_element_type=F32)
    return ghost.reshape(count, 8, 128)


SHARED = (1, 2, 4)


def plane_tiles(section):
    return NV if section == 3 else NV + -(-NV // SHARED[section])


def write_plane(plane, section, own, halo):
    for v in range(NV):
        plane[v] = own[v]
    if section == 3:
        return
    shared = SHARED[section]
    shift, need, sub = 8 // shared, 3 - section, subs()
    for start in range(0, NV, shared):
        tile = halo[start]
        for v in range(start + 1, min(start + shared, NV)):
            row = (sub + 8 - shift * (v - start)) % 8
            tile = jnp.where((row < need) | (row >= 8 - need), turn(halo[v], shift * (v - start), 0), tile)
        plane[NV + start // shared] = tile


def ghost_tile(ghost, section, v, half):
    if half == 0:
        return ghost[v]
    shared = SHARED[section]
    return turn(ghost[NV + v // shared], -(8 // shared) * (v % shared), 0)


def side_column(tile, other, own, west, is_rotor, swirl):
    lane, sub = lanes(), subs()
    far = turn(tile, -40)
    low_c, high_c = (far, own) if west else (own, far)
    up = turn(jnp.where(sub == 0, other, tile), 7, 0)
    down = turn(jnp.where(sub == 7, other, tile), 1, 0)
    ghost = turn(tile, -88)
    low = jnp.where(lane % CA == 0, jnp.where(is_rotor, ghost, 0.0), turn(tile, 1))
    high = jnp.where(lane % CA == CA - 1, jnp.where(is_rotor, 0.0, ghost), turn(tile, -1))
    part = jnp.where(lane < CA, turn(tile, -80), 0.0)
    e = part
    for var in range(1, NV):
        e = e + turn(part, CA * var)
    dc, dr, da = high_c - low_c, up - down, high - low
    lap = (high_c + low_c) + (up + down) + (high + low) - 6.0 * tile
    div = turn(dc, -CA) + turn(dr, -2 * CA) + turn(da, -3 * CA)
    flux = turn(div, 4 * CA)
    flux = jnp.where(lane < 4 * CA, turn(da, -CA), flux)
    flux = jnp.where(lane < 3 * CA, turn(dr, -2 * CA), flux)
    flux = jnp.where(lane < 2 * CA, turn(dc, -3 * CA), flux)
    flux = jnp.where(lane < CA, div, flux)
    return e * lap - (0.5 * swirl) * dc - (0.5 * AXIAL_MACH) * da - 0.5 * flux


def assemble(state, eddy, from_outer, from_inner, ext, eddy_ext, plane):
    upper = subs() < 4
    is_rotor = lax.axis_index("ax") == 1
    even_rad = is_even("rad")
    tiles = [[], []]
    for field in range(NV + 1):
        own_row, far_row = [], []
        for a in range(CA):
            pair = a // 2
            near, other = from_inner[field, pair], from_outer[field, pair]
            high = jnp.where(even_rad, near, other)
            low = jnp.where(even_rad, other, near)
            if a % 2 == 0:
                far = jnp.where(upper, high, pltpu.roll(low, 4, 0))
            else:
                far = jnp.where(upper, pltpu.roll(high, 4, 0), low)
            own = state[field, a] if field < NV else eddy[a]
            if field < NV:
                ext[field, a, 0:8] = own
                ext[field, a, 8:16] = far
            else:
                eddy_ext[a, 0:8] = own
                eddy_ext[a, 8:16] = far
            own_row.append(own)
            far_row.append(far)
        tiles[0].append(own_row)
        tiles[1].append(far_row)
    planes = [[jnp.where(is_rotor, row[0], row[CA - 1]) for row in tiles[half]] for half in range(2)]
    write_plane(plane, 0, *planes)


def section_kernel(section):
    last, first, paired = section == 3, section == 0, section % 2 == 0

    def kernel(*refs):
        refs = list(refs)
        field = refs.pop(0)
        base = field if first else refs.pop(0)
        acc_in = None if first else refs.pop(0)
        eddy = refs.pop(0)
        if paired:
            face, own_outer, own_inner, from_outer, from_inner = refs[:5]
            refs = refs[5:]
            start_outer, start_inner = (from_outer, from_inner) if first else (refs.pop(0), refs.pop(0))
            ghost = face[...]
        else:
            received, matrix, sides_in = refs[:3]
            refs = refs[3:]
            ghost = interpolated(received, matrix, section)
        if last:
            (out,) = refs
        elif paired:
            nxt, acc_out, plane, sides = refs
        else:
            nxt, acc_out, plane = refs
        lane, sub = lanes(), subs()
        even = is_even("circ")
        is_rotor = lax.axis_index("ax") == 1
        rad = lax.axis_index("rad")
        count = lax.axis_size("rad")
        swirl = jnp.where(is_rotor, F32(-0.3), F32(0.2))
        inside = jnp.where(sub < 4, jnp.where(rad == count - 1, 0.0, 1.0), jnp.where(rad == 0, 0.0, 1.0)).astype(F32)
        step = (0.5 * STEP, 0.5 * STEP, STEP, 0.0)[section]
        gain = STEP / 6.0 * (1.0, 2.0, 2.0, 1.0)[section]
        send_halves = {0: 2, 1: 2, 2: 1, 3: 0}[section]
        zero = jnp.zeros((8, 128), F32)

        def tile(v, a, half):
            return field[v, a, 8 * half : 8 * half + 8]

        def pick(near, beyond, half):
            rows = slice(8 * half, 8 * half + 8)
            x, y = near[rows], beyond[rows]
            return jnp.where(even, y, x), jnp.where(even, x, y)

        sides_now = []
        for half in range(1 if last else 2):
            rows = slice(8 * half, 8 * half + 8)
            sides_now.append(pick(from_inner, from_outer, half) if paired else (sides_in[0, rows], sides_in[1, rows]))
        moved = []
        for half in range(send_halves if paired else 0):
            own_last, own_first = pick(own_outer, own_inner, half)
            old = pick(start_inner, start_outer, half)
            for n, own in enumerate((own_first, own_last)):
                slope = side_column(sides_now[half][n], sides_now[1 - half][n], own, n == 0, is_rotor, swirl)
                moved.append((half, n, old[n] + step * (slope * inside if half == 1 else slope)))
        for half, n, value in moved:
            sides[n, 8 * half : 8 * half + 8] = value
        for half in range(1 if last else 2):
            rows = slice(8 * half, 8 * half + 8)
            west, east = sides_now[half]
            for a in range(CA):
                e = eddy[a, rows]
                dc, dr, da, lap = [], [], [], []
                for v in range(NV):
                    k = v * CA + a
                    c = tile(v, a, half)
                    o = tile(v, a, 1 - half)
                    cp = jnp.where(lane == 0, turn(west, -k), turn(c, 1))
                    cn = jnp.where(lane == 127, turn(east, 127 - k), turn(c, -1))
                    up = turn(jnp.where(sub == 0, o, c), 7, 0)
                    dn = turn(jnp.where(sub == 7, o, c), 1, 0)
                    g = ghost_tile(ghost, section, v, half)
                    lo = tile(v, a - 1, half) if a > 0 else jnp.where(is_rotor, g, zero)
                    hi = tile(v, a + 1, half) if a < CA - 1 else jnp.where(is_rotor, zero, g)
                    dc.append(cn - cp)
                    dr.append(up - dn)
                    da.append(hi - lo)
                    lap.append((cn + cp) + (up + dn) + (hi + lo) - 6.0 * c)
                div = 0.5 * (dc[1] + dr[2] + da[3])
                flux = (div, 0.5 * dc[4], 0.5 * dr[4], 0.5 * da[4], div)
                for v in range(NV):
                    slope = e * lap[v] - (0.5 * swirl) * dc[v] - (0.5 * AXIAL_MACH) * da[v] - flux[v]
                    if last:
                        out[v, a] = acc_in[v, a] + gain * slope
                        continue
                    if half == 1:
                        slope = slope * inside
                    u = base[v, a, rows] + step * slope
                    nxt[v, a, rows] = u
                    if half == 0:
                        acc_out[v, a] = (base[v, a, 0:8] if first else acc_in[v, a]) + gain * slope
        if not last:
            planes = [
                [jnp.where(is_rotor, nxt[v, 0, 8 * h : 8 * h + 8], nxt[v, CA - 1, 8 * h : 8 * h + 8]) for v in range(NV)]
                for h in range(2)
            ]
            write_plane(plane, section + 1, *planes)

    return kernel


def section_call(section, *args):
    if section == 3:
        return call(section_kernel(3), jax.ShapeDtypeStruct((NV, CA, 8, 128), F32), *args)
    rows = 8 if section == 2 else 16
    shapes = (sds(NV, CA, 16, 128), sds(NV, CA, 8, 128), sds(plane_tiles(section + 1), 8, 128))
    if section != 1:
        shapes += (sds(2, rows, 128),)
    return call(section_kernel(section), shapes, *args)


def inner_pairs(count):
    return [(i, i ^ 1) for i in range(count)]


def outer_pairs(count, wrap):
    pairs = [(i, i + 1 if i % 2 else i - 1) for i in range(count)]
    return [(i, j % count) for i, j in pairs if wrap or 0 <= j < count]


def same(source, out):
    out[...] = source[...]


def facing(plane, offset):
    count = lax.axis_size("circ")
    pairs = [(2 * ((c + offset) % count), 2 * c + 1) for c in range(count)]
    pairs += [(j, i) for i, j in pairs]
    ghost = lax.ppermute(plane, ("circ", "ax"), pairs)
    return call(same, sds(*ghost.shape), ghost)


def ghost_of(offset, plane):
    count = lax.axis_size("circ")
    return lax.switch(offset, [lambda p, o=o: facing(p, o) for o in range(count)], plane)


def beside(section, field, eddy, received, matrix):
    count = lax.axis_size("circ")
    shapes = (sds(plane_tiles(section), 8, 128), sds(16, 128), sds(16, 128))
    face, outer, inner = call(edges_kernel(section), shapes, field, eddy, received, matrix)
    from_outer = lax.ppermute(outer, "circ", outer_pairs(count, True))
    from_inner = lax.ppermute(inner, "circ", inner_pairs(count))
    return face, outer, inner, from_outer, from_inner


def local(state, eddy, offsets, stencil_index, stencil_weight):
    index = jnp.transpose(stencil_index, (0, 1, 3, 2))
    weight = jnp.transpose(stencil_weight, (0, 1, 3, 2))
    count = lax.axis_size("rad")
    message = sds(NV + 1, CA // 2, 8, 128)
    vmem = pl.BlockSpec(memory_space=pltpu.VMEM)
    inner, outer, own_state, own_eddy = pl.pallas_call(
        radial_out,
        in_specs=[pl.BlockSpec(memory_space=pl.ANY)] * 2,
        out_specs=(vmem,) * 4,
        out_shape=(message, message, sds(*state.shape), sds(*eddy.shape)),
        scratch_shapes=[pltpu.SemaphoreType.DMA((2,))],
        interpret=INTERPRET,
    )(state, eddy)
    from_outer = lax.ppermute(outer, "rad", outer_pairs(count, False))
    from_inner = lax.ppermute(inner, "rad", inner_pairs(count))
    matrix = call(matrices, sds(4, 128, 128), index, weight)
    places = [offsets[section] for section in range(4)]
    from_outer, from_inner, matrix, *places = lax.optimization_barrier((from_outer, from_inner, matrix, *places))
    ext, eddy_ext, plane = call(
        assemble,
        (sds(NV, CA, 16, 128), sds(CA, 16, 128), sds(plane_tiles(0), 8, 128)),
        own_state, own_eddy, from_outer, from_inner,
    )
    received = ghost_of(places[0], plane)
    edges = beside(0, ext, eddy_ext, received, matrix)
    field, acc, plane, sides = section_call(0, ext, eddy_ext, *edges)
    received = ghost_of(places[1], plane)
    field, acc, plane = section_call(1, field, ext, acc, eddy_ext, received, matrix, sides)
    received = ghost_of(places[2], plane)
    later = beside(2, field, eddy_ext, received, matrix)
    field, acc, plane, sides = section_call(2, field, ext, acc, eddy_ext, *later, *edges[3:])
    received = ghost_of(places[3], plane)
    return section_call(3, field, ext, acc, eddy_ext, received, matrix, sides)


def solution(mesh):
    return jax.shard_map(
        local,
        mesh=mesh,
        in_specs=(P(None, "ax", "rad", "circ"), P("ax", "rad", "circ"), P(), P(), P()),
        out_specs=P(None, "ax", "rad", "circ"),
        check_vma=False,
    )
```

```python
import jax
import jax.numpy as jnp
from jax import lax
from jax.experimental import pallas as pl
from jax.experimental.pallas import tpu as pltpu
from jax.sharding import PartitionSpec as P

NV = 5
CA = 8
AXIAL_MACH = 0.4
STEP = 0.3
F32 = jnp.float32
INTERPRET = False


def call(kernel, out_shape, *args):
    spec = pl.BlockSpec(memory_space=pltpu.VMEM)
    many = isinstance(out_shape, tuple)
    return pl.pallas_call(
        kernel,
        in_specs=[spec] * len(args),
        out_specs=(spec,) * len(out_shape) if many else spec,
        out_shape=out_shape,
        interpret=INTERPRET,
    )(*[pltpu.with_memory_space_constraint(a, pltpu.VMEM) for a in args])


def sds(*shape):
    return pltpu.VMEM(shape, F32)


def lanes():
    return lax.broadcasted_iota(jnp.int32, (8, 128), 1)


def subs():
    return lax.broadcasted_iota(jnp.int32, (8, 128), 0)


def is_even(axis):
    return lax.axis_index(axis) % 2 == 0


def radial_out(state_in, eddy_in, inner, outer, state, eddy, done):
    copies = [
        pltpu.make_async_copy(state_in, state, done.at[0]),
        pltpu.make_async_copy(eddy_in, eddy, done.at[1]),
    ]
    for copy in copies:
        copy.start()
    for copy in copies:
        copy.wait()
    upper = subs() < 4
    even_rad = is_even("rad")
    for field in range(NV + 1):
        for pair in range(CA // 2):
            if field < NV:
                even, odd = state[field, 2 * pair], state[field, 2 * pair + 1]
            else:
                even, odd = eddy[2 * pair], eddy[2 * pair + 1]
            to_low = jnp.where(upper, even, pltpu.roll(odd, 4, 0))
            to_high = jnp.where(upper, pltpu.roll(even, 4, 0), odd)
            inner[field, pair] = jnp.where(even_rad, to_high, to_low)
            outer[field, pair] = jnp.where(even_rad, to_low, to_high)


def matrices(index, weight, out):
    side = lax.axis_index("ax")
    rows = lax.broadcasted_iota(jnp.int32, (128, 128), 0)
    for section in range(4):
        taps_at = index[side, section]
        weights = weight[side, section]
        weights = weights / jnp.sum(weights, axis=0, keepdims=True)
        total = jnp.zeros((128, 128), F32)
        for tap in range(4):
            total = total + jnp.where(rows == taps_at[tap : tap + 1], weights[tap : tap + 1], 0.0)
        out[section] = total


def edges_kernel(section):
    def kernel(field, eddy, received, matrix, face, outer, inner):
        ghost = interpolated(received, matrix, section)
        face[...] = ghost
        for half in range(2):
            rows = slice(8 * half, 8 * half + 8)
            first = jnp.zeros((8, 128), F32)
            last = jnp.zeros((8, 128), F32)
            for var in range(NV):
                for a in range(CA):
                    k = var * CA + a
                    x = field[var, a, rows]
                    first = place(first, x, 0, k)
                    first = place(first, x, 1, 40 + k)
                    last = place(last, x, 127, k)
                    last = place(last, x, 126, 40 + k)
            for a in range(CA):
                first = place(first, eddy[a, rows], 0, 80 + a)
                last = place(last, eddy[a, rows], 127, 80 + a)
            for var in range(NV):
                for a in (0, CA - 1):
                    k = 88 + var * CA + a
                    first = place(first, ghost_tile(ghost, section, var, half), 0, k)
                    last = place(last, ghost_tile(ghost, section, var, half), 127, k)
            inner[rows] = last
            outer[rows] = first

    return kernel


def turn(x, amount, axis=1):
    amount %= x.shape[axis]
    return pltpu.roll(x, amount, axis) if amount else x


def place(tile, x, source, target):
    return jnp.where(lanes() == target, turn(x, target - source), tile)


def interpolated(received, matrix, section):
    count = received.shape[0]
    flat = received[...].reshape(count * 8, 128)
    ghost = jnp.dot(flat, matrix[section], precision=lax.Precision.HIGHEST, preferred_element_type=F32)
    return ghost.reshape(count, 8, 128)


SHARED = (1, 2, 4)


def plane_tiles(section):
    return NV if section == 3 else NV + -(-NV // SHARED[section])


def write_plane(plane, section, own, halo):
    for v in range(NV):
        plane[v] = own[v]
    if section == 3:
        return
    shared = SHARED[section]
    shift, need, sub = 8 // shared, 3 - section, subs()
    for start in range(0, NV, shared):
        tile = halo[start]
        for v in range(start + 1, min(start + shared, NV)):
            row = (sub + 8 - shift * (v - start)) % 8
            tile = jnp.where((row < need) | (row >= 8 - need), turn(halo[v], shift * (v - start), 0), tile)
        plane[NV + start // shared] = tile


def ghost_tile(ghost, section, v, half):
    if half == 0:
        return ghost[v]
    shared = SHARED[section]
    return turn(ghost[NV + v // shared], -(8 // shared) * (v % shared), 0)


def side_column(tile, other, own, west, is_rotor, swirl):
    lane, sub = lanes(), subs()
    far = turn(tile, -40)
    low_c, high_c = (far, own) if west else (own, far)
    up = turn(jnp.where(sub == 0, other, tile), 7, 0)
    down = turn(jnp.where(sub == 7, other, tile), 1, 0)
    ghost = turn(tile, -88)
    low = jnp.where(lane % CA == 0, jnp.where(is_rotor, ghost, 0.0), turn(tile, 1))
    high = jnp.where(lane % CA == CA - 1, jnp.where(is_rotor, 0.0, ghost), turn(tile, -1))
    part = jnp.where(lane < CA, turn(tile, -80), 0.0)
    e = part
    for var in range(1, NV):
        e = e + turn(part, CA * var)
    dc, dr, da = high_c - low_c, up - down, high - low
    lap = (high_c + low_c) + (up + down) + (high + low) - 6.0 * tile
    div = turn(dc, -CA) + turn(dr, -2 * CA) + turn(da, -3 * CA)
    flux = turn(div, 4 * CA)
    flux = jnp.where(lane < 4 * CA, turn(da, -CA), flux)
    flux = jnp.where(lane < 3 * CA, turn(dr, -2 * CA), flux)
    flux = jnp.where(lane < 2 * CA, turn(dc, -3 * CA), flux)
    flux = jnp.where(lane < CA, div, flux)
    return e * lap - (0.5 * swirl) * dc - (0.5 * AXIAL_MACH) * da - 0.5 * flux


def assemble(state, eddy, from_outer, from_inner, ext, eddy_ext, plane):
    upper = subs() < 4
    is_rotor = lax.axis_index("ax") == 1
    even_rad = is_even("rad")
    tiles = [[], []]
    for field in range(NV + 1):
        own_row, far_row = [], []
        for a in range(CA):
            pair = a // 2
            near, other = from_inner[field, pair], from_outer[field, pair]
            high = jnp.where(even_rad, near, other)
            low = jnp.where(even_rad, other, near)
            if a % 2 == 0:
                far = jnp.where(upper, high, pltpu.roll(low, 4, 0))
            else:
                far = jnp.where(upper, pltpu.roll(high, 4, 0), low)
            own = state[field, a] if field < NV else eddy[a]
            if field < NV:
                ext[field, a, 0:8] = own
                ext[field, a, 8:16] = far
            else:
                eddy_ext[a, 0:8] = own
                eddy_ext[a, 8:16] = far
            own_row.append(own)
            far_row.append(far)
        tiles[0].append(own_row)
        tiles[1].append(far_row)
    planes = [[jnp.where(is_rotor, row[0], row[CA - 1]) for row in tiles[half]] for half in range(2)]
    write_plane(plane, 0, *planes)


def section_kernel(section):
    last, first, paired = section == 3, section == 0, section % 2 == 0

    def kernel(*refs):
        refs = list(refs)
        field = refs.pop(0)
        base = field if first else refs.pop(0)
        acc_in = None if first else refs.pop(0)
        eddy = refs.pop(0)
        if paired:
            face, own_outer, own_inner, from_outer, from_inner = refs[:5]
            refs = refs[5:]
            start_outer, start_inner = (from_outer, from_inner) if first else (refs.pop(0), refs.pop(0))
            ghost = face[...]
        else:
            received, matrix, sides_in = refs[:3]
            refs = refs[3:]
            ghost = interpolated(received, matrix, section)
        if last:
            (out,) = refs
        elif paired:
            nxt, acc_out, plane, sides = refs
        else:
            nxt, acc_out, plane = refs
        lane, sub = lanes(), subs()
        is_rotor = lax.axis_index("ax") == 1
        rad = lax.axis_index("rad")
        count = lax.axis_size("rad")
        swirl = jnp.where(is_rotor, F32(-0.3), F32(0.2))
        inside = jnp.where(sub < 4, jnp.where(rad == count - 1, 0.0, 1.0), jnp.where(rad == 0, 0.0, 1.0)).astype(F32)
        step = (0.5 * STEP, 0.5 * STEP, STEP, 0.0)[section]
        gain = STEP / 6.0 * (1.0, 2.0, 2.0, 1.0)[section]
        send_halves = {0: 2, 1: 2, 2: 1, 3: 0}[section]
        zero = jnp.zeros((8, 128), F32)

        def tile(v, a, half):
            return field[v, a, 8 * half : 8 * half + 8]

        def pick(near, beyond, half):
            rows = slice(8 * half, 8 * half + 8)
            x, y = near[rows], beyond[rows]
            return y, x

        sides_now = []
        for half in range(1 if last else 2):
            rows = slice(8 * half, 8 * half + 8)
            sides_now.append(pick(from_inner, from_outer, half) if paired else (sides_in[0, rows], sides_in[1, rows]))
        moved = []
        for half in range(send_halves if paired else 0):
            own_last, own_first = pick(own_outer, own_inner, half)
            old = pick(start_inner, start_outer, half)
            for n, own in enumerate((own_first, own_last)):
                slope = side_column(sides_now[half][n], sides_now[1 - half][n], own, n == 0, is_rotor, swirl)
                moved.append((half, n, old[n] + step * (slope * inside if half == 1 else slope)))
        for half, n, value in moved:
            sides[n, 8 * half : 8 * half + 8] = value
        for half in range(1 if last else 2):
            rows = slice(8 * half, 8 * half + 8)
            west, east = sides_now[half]
            for a in range(CA):
                e = eddy[a, rows]
                dc, dr, da, lap = [], [], [], []
                for v in range(NV):
                    k = v * CA + a
                    c = tile(v, a, half)
                    o = tile(v, a, 1 - half)
                    cp = jnp.where(lane == 0, turn(west, -k), turn(c, 1))
                    cn = jnp.where(lane == 127, turn(east, 127 - k), turn(c, -1))
                    up = turn(jnp.where(sub == 0, o, c), 7, 0)
                    dn = turn(jnp.where(sub == 7, o, c), 1, 0)
                    g = ghost_tile(ghost, section, v, half)
                    lo = tile(v, a - 1, half) if a > 0 else jnp.where(is_rotor, g, zero)
                    hi = tile(v, a + 1, half) if a < CA - 1 else jnp.where(is_rotor, zero, g)
                    dc.append(cn - cp)
                    dr.append(up - dn)
                    da.append(hi - lo)
                    lap.append((cn + cp) + (up + dn) + (hi + lo) - 6.0 * c)
                div = 0.5 * (dc[1] + dr[2] + da[3])
                flux = (div, 0.5 * dc[4], 0.5 * dr[4], 0.5 * da[4], div)
                for v in range(NV):
                    slope = e * lap[v] - (0.5 * swirl) * dc[v] - (0.5 * AXIAL_MACH) * da[v] - flux[v]
                    if last:
                        out[v, a] = acc_in[v, a] + gain * slope
                        continue
                    if half == 1:
                        slope = slope * inside
                    u = base[v, a, rows] + step * slope
                    nxt[v, a, rows] = u
                    if half == 0:
                        acc_out[v, a] = (base[v, a, 0:8] if first else acc_in[v, a]) + gain * slope
        if not last:
            planes = [
                [jnp.where(is_rotor, nxt[v, 0, 8 * h : 8 * h + 8], nxt[v, CA - 1, 8 * h : 8 * h + 8]) for v in range(NV)]
                for h in range(2)
            ]
            write_plane(plane, section + 1, *planes)

    return kernel


def section_call(section, *args):
    if section == 3:
        return call(section_kernel(3), jax.ShapeDtypeStruct((NV, CA, 8, 128), F32), *args)
    rows = 8 if section == 2 else 16
    shapes = (sds(NV, CA, 16, 128), sds(NV, CA, 8, 128), sds(plane_tiles(section + 1), 8, 128))
    if section != 1:
        shapes += (sds(2, rows, 128),)
    return call(section_kernel(section), shapes, *args)


def inner_pairs(count):
    return [(i, i ^ 1) for i in range(count)]


def outer_pairs(count, wrap):
    pairs = [(i, i + 1 if i % 2 else i - 1) for i in range(count)]
    return [(i, j % count) for i, j in pairs if wrap or 0 <= j < count]


def same(source, out):
    out[...] = source[...]


def facing(plane, offset):
    count = lax.axis_size("circ")
    pairs = [(2 * ((c + offset) % count), 2 * c + 1) for c in range(count)]
    pairs += [(j, i) for i, j in pairs]
    ghost = lax.ppermute(plane, ("circ", "ax"), pairs)
    return call(same, sds(*ghost.shape), ghost)


def ghost_of(offset, plane):
    count = lax.axis_size("circ")
    return lax.switch(offset, [lambda p, o=o: facing(p, o) for o in range(count)], plane)


def beside(section, field, eddy, received, matrix):
    count = lax.axis_size("circ")
    shapes = (sds(plane_tiles(section), 8, 128), sds(16, 128), sds(16, 128))
    face, outer, inner = call(edges_kernel(section), shapes, field, eddy, received, matrix)
    to_east = [(i, (i + 1) % count) for i in range(count)]
    from_outer = lax.ppermute(inner, "circ", to_east)
    from_inner = lax.ppermute(outer, "circ", [(j, i) for i, j in to_east])
    return face, outer, inner, from_outer, from_inner


def local(state, eddy, offsets, stencil_index, stencil_weight):
    index = jnp.transpose(stencil_index, (0, 1, 3, 2))
    weight = jnp.transpose(stencil_weight, (0, 1, 3, 2))
    count = lax.axis_size("rad")
    message = sds(NV + 1, CA // 2, 8, 128)
    vmem = pl.BlockSpec(memory_space=pltpu.VMEM)
    inner, outer, own_state, own_eddy = pl.pallas_call(
        radial_out,
        in_specs=[pl.BlockSpec(memory_space=pl.ANY)] * 2,
        out_specs=(vmem,) * 4,
        out_shape=(message, message, sds(*state.shape), sds(*eddy.shape)),
        scratch_shapes=[pltpu.SemaphoreType.DMA((2,))],
        interpret=INTERPRET,
    )(state, eddy)
    from_outer = lax.ppermute(outer, "rad", outer_pairs(count, False))
    from_inner = lax.ppermute(inner, "rad", inner_pairs(count))
    matrix = call(matrices, sds(4, 128, 128), index, weight)
    places = [offsets[section] for section in range(4)]
    from_outer, from_inner, matrix, *places = lax.optimization_barrier((from_outer, from_inner, matrix, *places))
    ext, eddy_ext, plane = call(
        assemble,
        (sds(NV, CA, 16, 128), sds(CA, 16, 128), sds(plane_tiles(0), 8, 128)),
        own_state, own_eddy, from_outer, from_inner,
    )
    received = ghost_of(places[0], plane)
    edges = beside(0, ext, eddy_ext, received, matrix)
    field, acc, plane, sides = section_call(0, ext, eddy_ext, *edges)
    received = ghost_of(places[1], plane)
    field, acc, plane = section_call(1, field, ext, acc, eddy_ext, received, matrix, sides)
    received = ghost_of(places[2], plane)
    later = beside(2, field, eddy_ext, received, matrix)
    field, acc, plane, sides = section_call(2, field, ext, acc, eddy_ext, *later, *edges[3:])
    received = ghost_of(places[3], plane)
    return section_call(3, field, ext, acc, eddy_ext, received, matrix, sides)


def solution(mesh):
    return jax.shard_map(
        local,
        mesh=mesh,
        in_specs=(P(None, "ax", "rad", "circ"), P("ax", "rad", "circ"), P(), P(), P()),
        out_specs=P(None, "ax", "rad", "circ"),
        check_vma=False,
    )
```
